32 devices in a mesh: groups: 2 (over x), head: 8 (over z, y), seq: 2 (over core).
Axes of the slice: x: 2, y: 2, z: 4, core: 2. Of those that a mesh axis runs over, the one named last changes fastest.
Arguments:
- hidden: bfloat16 [768, 7168], P(('groups', 'head', 'seq')), parts along dimension 0, may hold values from -6 to 6
- query_latent: bfloat16 [768, 1536], P(('groups', 'head', 'seq')), parts along dimension 0, may hold values from -240 to 240
- kv_down: bfloat16 [7168, 576], P('seq'), may hold values from -0.0625 to 0.0625
- kv_gain: float32 [512], replicated, may hold values from 0.25 to 1.75
- q_up: bfloat16 [1536, 24576], P(None, 'head'), may hold values from -0.15625 to 0.15625
- k_up: bfloat16 [512, 16384], P(None, 'head'), may hold values from -0.25 to 0.25
- v_up: bfloat16 [512, 16384], P(None, 'head'), may hold values from -0.25 to 0.25
- out_proj: bfloat16 [16384, 7168], P('head', 'seq'), may hold values from -0.125 to 0.125
- block_order: int32 [32], P('groups'), parts along dimension 0, may hold values from 0 to 15, each once
Outputs:
- attn_out: bfloat16 [768, 7168], P(('groups', 'head', 'seq')), parts along dimension 0
The draws below stay inside these ranges and needn't reach their ends.
There are 2 independent parts, one for each index of `groups`. The reference program is written for one: setup_inputs(seed, part) draws one part's arguments, and reference() takes and returns one part's arrays. A program takes and returns all parts, laid end to end along the dimension named above; an argument that names none is the same for every part. Nothing has to cross between parts.
Inputs may be any that keep to these rules, and one draw needn't show every extreme that they name: Each of 0 to 15 once; stored rows j * 24 to (j + 1) * 24 - 1 hold the positions block_order[j] * 24 onwards, in order.
All inputs are finite; a program needn't handle non-finite values.
Results may differ from the reference program's by a relative error of at most 0.025.
Values may be sent and summed in bfloat16 or wider, within the bound.
A program may use at most 128 MiB of HBM per device.

```python
import jax
import jax.numpy as jnp
from jax import lax

D = 7168
HEADS = 128
LATENT = 512
ROPE = 64
NOPE = 128
VDIM = 128
QLAT = 1536
TOK_DEV = 24
BLOCKS = 16
LENGTH = 384
N_HEAD = 8


def draw_query_latent(key, part):
    key_base = jax.random.fold_in(key, 11)
    result = jnp.clip(2.0 * jax.random.normal(key_base, (LENGTH, QLAT), jnp.float32), -12.0, 12.0)
    return result.astype(jnp.bfloat16)


def block_scale(rng, shape, pieces, least, high):
    def one(axis_at, parts):
        steps = jax.random.uniform(jax.random.fold_in(jax.random.fold_in(rng, 6), axis_at), (parts,), jnp.float32, least / len(pieces), high / len(pieces))
        return jnp.repeat(jnp.exp(steps), shape[axis_at] // parts).reshape((-1,) + (1,) * (len(shape) - axis_at - 1))

    factor_of = one(*pieces[0])
    for cut in pieces[1:]:
        factor_of = factor_of * one(*cut)
    return factor_of


def bell_draw(key, dims, scale, reach, split=(), kind=jnp.bfloat16):
    values = jax.random.normal(key, dims, jnp.float32) * scale
    if len(split) > 0:
        values = block_scale(key, dims, split, -0.22, 0.18) * values
    return jnp.clip(values, min=-reach, max=reach).astype(kind)


def setup_inputs(seed: int = 0, part: int = 0) -> dict:
    keys = jax.random.split(jax.random.key(seed), 10)
    own_keys = jax.random.split(jax.random.fold_in(keys[9], part), 10)
    hidden = bell_draw(own_keys[0], (LENGTH, D), 1.0, 6.0, ((0, 16),))
    query_latent = draw_query_latent(jax.random.fold_in(jax.random.fold_in(keys[9], part), 71), part)
    kv_down = bell_draw(keys[2], (D, LATENT + ROPE), D ** -0.5, 0.0625, ((0, 2),))
    kv_gain = jnp.clip(1.0 + 0.15 * jax.random.normal(keys[3], (LATENT,), jnp.float32), 0.25, 1.75)
    q_up = bell_draw(keys[4], (QLAT, HEADS * (NOPE + ROPE)), QLAT ** -0.5, 0.15625, ((1, 8),))
    k_up = bell_draw(keys[5], (LATENT, HEADS * NOPE), LATENT ** -0.5, 0.25, ((1, 8),))
    v_up = bell_draw(keys[6], (LATENT, HEADS * VDIM), LATENT ** -0.5, 0.25, ((1, 8),))
    out_proj = bell_draw(keys[7], (HEADS * VDIM, D), (HEADS * VDIM // 8) ** -0.5, 0.125, ((0, 8), (1, 2)))
    block_order = jax.random.permutation(own_keys[8], BLOCKS).astype(jnp.int32)
    return {"hidden": hidden, "query_latent": query_latent, "kv_down": kv_down, "kv_gain": kv_gain, "q_up": q_up, "k_up": k_up, "v_up": v_up, "out_proj": out_proj, "block_order": block_order}


EPSILON = 1e-06
THETA = 10000.0
MASKED = -1e+30

def rotate(values, positions):
    half_width = values.shape[-1] // 2
    frequency = THETA ** (-jnp.arange(half_width, dtype=jnp.float32) / half_width)
    angles = positions.astype(jnp.float32)[:, None] * frequency[None, :]
    shaped = (values.shape[0],) + (1,) * (values.ndim - 2) + (half_width,)
    cosine = jnp.cos(angles).reshape(shaped)
    sine_table = jnp.sin(angles).reshape(shaped)
    front_part = values[..., :half_width]
    back_part = values[..., half_width:]
    return jnp.concatenate([front_part * cosine - back_part * sine_table, front_part * sine_table + back_part * cosine], axis=-1)

def reference(hidden, query_latent, kv_down, kv_gain, q_up, k_up, v_up, out_proj, block_order):
    row_index = jnp.arange(LENGTH, dtype=jnp.int32)
    positions = block_order[row_index // TOK_DEV] * TOK_DEV + row_index % TOK_DEV
    latent_raw = jnp.dot(hidden, kv_down, preferred_element_type=jnp.float32)
    compressed = latent_raw[:, :LATENT]
    mean_square = lax.optimization_barrier(jnp.mean(compressed * compressed, axis=-1, keepdims=True))
    kv_part = (compressed * lax.rsqrt(mean_square + EPSILON) * kv_gain).astype(jnp.bfloat16)
    rope_keys = rotate(latent_raw[:, LATENT:], positions).astype(jnp.bfloat16)
    scaling = (NOPE + ROPE) ** (-0.5)
    projected = jnp.dot(query_latent, q_up, preferred_element_type=jnp.float32).reshape(LENGTH, HEADS, NOPE + ROPE)
    queries = (jnp.concatenate([projected[..., :NOPE], rotate(projected[..., NOPE:], positions)], axis=-1) * scaling).astype(jnp.bfloat16)
    key_rows = jnp.dot(kv_part, k_up, preferred_element_type=jnp.float32).astype(jnp.bfloat16).reshape(LENGTH, HEADS, NOPE)
    value_rows = jnp.dot(kv_part, v_up, preferred_element_type=jnp.float32).astype(jnp.bfloat16).reshape(LENGTH, HEADS, VDIM)
    allowed = positions[None, :] <= positions[:, None]

    def one_head(operands):
        query_head, key_head, value_head = operands
        scores = jnp.dot(query_head[:, :NOPE], key_head.T, preferred_element_type=jnp.float32)
        scores = scores + jnp.dot(query_head[:, NOPE:], rope_keys.T, preferred_element_type=jnp.float32)
        scores = jnp.where(allowed, scores, MASKED)
        row_max = lax.optimization_barrier(jnp.max(scores, axis=-1, keepdims=True))
        weights = jnp.where(allowed, jnp.exp(scores - row_max), 0.0)
        totals = lax.optimization_barrier(jnp.sum(weights, axis=-1, keepdims=True))
        mixture = jnp.dot(weights.astype(jnp.bfloat16), value_head, preferred_element_type=jnp.float32) / totals
        return mixture.astype(jnp.bfloat16)
    heads_out = lax.map(one_head, (queries.transpose(1, 0, 2), key_rows.transpose(1, 0, 2), value_rows.transpose(1, 0, 2)))
    group_heads = HEADS // N_HEAD
    grouped_out = heads_out.reshape(N_HEAD, group_heads, LENGTH, VDIM)
    grouped_proj = out_proj.reshape(N_HEAD, group_heads * VDIM, D)

    def add_group(running, operands):
        head_block, proj_block = operands
        head_rows = head_block.transpose(1, 0, 2).reshape(LENGTH, group_heads * VDIM)
        partial_sum = jnp.dot(head_rows, proj_block, preferred_element_type=jnp.float32)
        rounded = lax.optimization_barrier(partial_sum.astype(jnp.bfloat16))
        return (running + rounded.astype(jnp.float32), None)
    summed, unused = lax.scan(add_group, jnp.zeros((LENGTH, D), jnp.float32), (grouped_out, grouped_proj))
    return summed.astype(jnp.bfloat16)
```

```python
import functools

import jax
import jax.numpy as jnp
import numpy as np
from jax import lax
from jax.experimental import pallas as pl
from jax.experimental.pallas import tpu as pltpu
from jax.sharding import PartitionSpec as P

ROPE = 64
NOPE = 128
VDIM = 128


EPSILON = 1e-06
THETA = 10000.0
MASKED = -1e30


MESH = pl.DeviceIdType.MESH
CHUNK = 256
LANES = 128
VMEM_BYTES = 67043328


def bit_orders(bits, chunks):
    plain = list(range(bits))
    if bits < 3:
        return [plain] * chunks
    other = [1, 0] + plain[2:]
    return [other if chunk % 7 in (1, 4) else plain for chunk in range(chunks)]


def plan(bits, chunks, orders):
    compute, latency, unit = 0.55, 2.2, 4.3
    clock, free, events, now = 0.0, {}, [], 0.0
    ready = {}
    pending = [(compute * (c + 1), c, 0) for c in range(chunks)]
    while pending:
        pending.sort()
        when, chunk, step = pending.pop(0)
        events.append((chunk, step))
        if step < bits:
            bit = orders[chunk][step]
            start = max(when, free.get(bit, 0.0))
            wire = unit / 2 ** (step + 1) * (2 if bit > 1 else 1)
            free[bit] = start + wire
            pending.append((start + wire + latency, chunk, step + 1))
    return events


def gather_orders(bits):
    far = list(range(bits))[::-1]
    near = far[:-2] + far[-2:][::-1]
    return [near, near, far]


def turn(x, cosine, up, down):
    return x * cosine + pltpu.roll(x, ROPE // 2, 1) * up + pltpu.roll(x, LANES - ROPE // 2, 1) * down


def angle_table(places):
    lane = np.arange(LANES)
    rotary = ROPE // 2
    rate = np.where(lane < ROPE, THETA ** (-(lane % rotary) / rotary), 0.0)
    angles = places[:, None] * rate
    return jnp.asarray(np.concatenate([np.cos(angles), np.sin(angles)], axis=1), jnp.float32)


def layer_kernel(bits, chunks, orders, *refs):
    (
        order_ref, hidden_hbm, query_hbm, kv_down, gain_hbm, q_up, k_up, v_up, out_proj,
        blocks_hbm, within_hbm, o_ref,
        hidden, query, gain, blocks, within, cosine, up, down,
        kv_vmem, q_vmem, k_vmem, v_vmem, w_vmem,
        raw_out, raw_in, ql, lat, q_rows, rows, kv, tail_a, tail_b, bias,
        heads, heads_in, x32, x, part,
    ) = refs[:40]
    rest = refs[40:]
    recvs = rest[:bits]
    (
        mine, theirs, landed,
        in_sem, first_sem, q_sem, k_sem, v_sem, w_sem,
        send_sem, recv_sem, swap_sem, ql_sem, lat_sem, head_sem,
    ) = rest[bits:]
    head = lax.axis_index("head")
    seq = lax.axis_index("seq")
    digit = [(head // 2**bit) % 2 for bit in range(bits)]
    partner = [head + 2**bit * (1 - 2 * digit[bit]) for bit in range(bits)]
    tok = o_ref.shape[0]
    half = out_proj.shape[1]
    depth = kv_down.shape[1]
    pairs = q_vmem.shape[0]
    count = 2**bits
    width = kv.shape[1]
    f32, bf16 = jnp.float32, jnp.bfloat16

    def loader(src, dst, sem, size):
        def at(p):
            columns = pl.ds(p * size, size)
            return pltpu.make_async_copy(src.at[:, columns], dst.at[p], sem.at[p])

        return at

    load_q = loader(q_up, q_vmem, q_sem, 2 * (NOPE + ROPE))
    load_k = loader(k_up, k_vmem, k_sem, 2 * NOPE)
    load_v = loader(v_up, v_vmem, v_sem, 2 * VDIM)
    load_w = loader(out_proj, w_vmem, w_sem, CHUNK)
    load_kv = pltpu.make_async_copy(kv_down, kv_vmem, in_sem.at[0])

    mine_side = pl.multiple_of(seq * depth, 128)
    their_side = pl.multiple_of((1 - seq) * depth, 128)
    first = [
        pltpu.make_async_copy(src, dst, first_sem.at[k])
        for k, (src, dst) in enumerate(
            (
                (hidden_hbm.at[:, pl.ds(their_side, depth)], hidden.at[pl.ds(2 * tok, tok)]),
                (query_hbm, query),
                (hidden_hbm.at[:, pl.ds(mine_side, depth)], hidden.at[pl.ds(0, tok)]),
                (gain_hbm, gain),
                (blocks_hbm, blocks),
                (within_hbm, within),
            )
        )
    ]
    for copy in first:
        copy.start()
    load_kv.start()
    for p in range(pairs):
        load_q(p).start()
    barrier = pltpu.get_barrier_semaphore()
    for bit in range(bits):
        pl.semaphore_signal(
            barrier, inc=1, device_id={"head": partner[bit]}, device_id_type=MESH
        )
    pl.semaphore_signal(barrier, inc=1, device_id={"seq": 1 - seq}, device_id_type=MESH)
    pl.semaphore_wait(barrier, bits + 1)

    def swap(src, dst, sem, k):
        return pltpu.make_async_remote_copy(
            src_ref=src,
            dst_ref=dst,
            send_sem=sem.at[0, k],
            recv_sem=sem.at[1, k],
            device_id={"seq": 1 - seq},
            device_id_type=MESH,
        )

    def to_head(src, dst, sem, step, k, bit):
        return pltpu.make_async_remote_copy(
            src_ref=src,
            dst_ref=dst,
            send_sem=sem.at[0, step, k],
            recv_sem=sem.at[1, step, k],
            device_id={"head": partner[bit]},
            device_id_type=MESH,
        )

    def place(order, step):
        done = order[:step]
        return tuple(slice(None) if bit in done else digit[bit] for bit in reversed(range(bits)))

    piece_orders = gather_orders(bits)
    pieces = len(piece_orders)
    piece = query.shape[1] // pieces

    def ql_copy(p, step):
        order = piece_orders[p]
        target = ql.at[(p,) + place(order, step)]
        source = query.at[:, pl.ds(p * piece, piece)] if step == 0 else target
        return to_head(source, target, ql_sem, step, p, order[step])

    lat_order = piece_orders[-1]

    def lat_copy(step):
        target = lat.at[(seq,) + place(lat_order, step)]
        return to_head(target, target, lat_sem, step, 0, lat_order[step])

    hid_swap = swap(hidden.at[pl.ds(2 * tok, tok)], hidden.at[pl.ds(tok, tok)], swap_sem, 0)
    raw_swap = swap(raw_out, raw_in, swap_sem, 1)
    lat_swap = swap(lat.at[seq], lat.at[seq], swap_sem, 2)
    end_swap = swap(theirs, landed, swap_sem, 3)
    first[0].wait()
    hid_swap.start()
    first[1].wait()
    for p in range(pieces):
        ql_copy(p, 0).start()
    for p in range(pairs):
        load_k(p).start()
        load_v(p).start()
    for p in range(pieces):
        ql[(p,) + place(lat_order, 0)] = query[:, pl.ds(p * piece, piece)]

    for copy in first[2:]:
        copy.wait()
    lane = lax.broadcasted_iota(jnp.int32, (tok, LANES), 1)
    rotary = ROPE // 2
    for j in range(count):
        stored = order_ref[j * 2 + seq]
        one = blocks[pl.ds(stored, 1), :]
        block_cos, block_sin = one[:, :LANES], one[:, LANES:]
        row_cos, row_sin = within[:, :LANES], within[:, LANES:]
        sine = block_sin * row_cos + block_cos * row_sin
        at = pl.ds(j * tok, tok)
        cosine[at, :] = block_cos * row_cos - block_sin * row_sin
        up[at, :] = jnp.where(lane >= rotary, sine, 0.0)
        down[at, :] = jnp.where(lane < rotary, -sine, 0.0)
    load_kv.wait()
    hid_swap.wait_recv()
    raw_all = lax.dot_general(
        hidden[: 2 * tok, :], kv_vmem[...], (((1,), (1,)), ((), ())), preferred_element_type=f32
    )
    raw_out[...] = raw_all[tok:]
    raw_swap.start()
    keys_all = 2 * count * tok
    spot = lax.broadcasted_iota(jnp.int32, (8, keys_all), 1)
    key_pos = spot
    for k in range(2 * count):
        side, j = k // count, k % count
        shift = (order_ref[j * 2 + side] - k) * tok
        key_pos = key_pos + jnp.where((spot >= k * tok) & (spot < (k + 1) * tok), shift, 0)
    for j in range(count):
        row = order_ref[j * 2 + seq] * tok + lax.broadcasted_iota(jnp.int32, (tok, keys_all), 0)
        seen = jnp.concatenate([key_pos] * (tok // 8), axis=0) <= row
        bias[pl.ds(j * tok, tok), :] = jnp.where(seen, 0.0, MASKED).astype(bf16)
    raw_swap.wait_recv()
    raw = raw_all[:tok] + raw_in[...]
    compressed = raw[:, :width]
    square = jnp.mean(compressed * compressed, axis=-1, keepdims=True)
    own = pl.ds(pl.multiple_of(head * tok, 8), tok)
    rope = jnp.concatenate([raw[:, width:], jnp.zeros((tok, LANES - ROPE), f32)], axis=1)
    rope = turn(rope, cosine[own, :], up[own, :], down[own, :])
    normed = compressed * lax.rsqrt(square + EPSILON) * gain[...]
    lat[(seq,) + place(lat_order, 0)] = jnp.concatenate([normed, rope], axis=1).astype(bf16)
    lat_copy(0).start()

    for step in range(1, bits):
        for p in range(pieces):
            ql_copy(p, step - 1).wait_recv()
            ql_copy(p, step).start()
        lat_copy(step - 1).wait_recv()
        lat_copy(step).start()
    for p in range(pieces):
        ql_copy(p, bits - 1).wait_recv()
        block = ql[p].astype(f32).reshape(count * tok, piece)
        rows[:, pl.ds(p * piece, piece)] = block.astype(bf16)

    scaling = (NOPE + ROPE) ** (-0.5)

    def project_query(p, carry):
        load_q(p).wait()
        got = jnp.dot(rows[...], q_vmem[p], preferred_element_type=f32)
        tables = (cosine[...], up[...], down[...])
        first = turn(got[:, LANES : 2 * LANES], *tables)
        last = turn(got[:, 2 * LANES :], *(pltpu.roll(t, ROPE, 1) for t in tables))
        q_rows[p, :, :LANES] = (got[:, :LANES] * scaling).astype(bf16)
        q_rows[p, :, LANES : 2 * LANES] = (first * scaling).astype(bf16)
        q_rows[p, :, 2 * LANES :] = (last * scaling).astype(bf16)
        return carry

    lax.fori_loop(0, pairs, project_query, 0)
    lat_copy(bits - 1).wait_recv()
    lat_swap.start()
    for c in range(chunks):
        load_w(c).start()

    def unpack(side):
        at = pl.ds(pl.multiple_of(side * count * tok, 8 * tok), count * tok)
        keys = lat[side].astype(f32).reshape(count * tok, width + LANES)
        kv[at, :] = keys[:, :width].astype(bf16)
        tail_a[at, :] = keys[:, width:].astype(bf16)
        tail_b[at, :] = pltpu.roll(keys[:, width:], ROPE, 1)

    unpack(seq)
    swap(lat.at[1 - seq], lat.at[1 - seq], swap_sem, 2).wait_recv()
    unpack(1 - seq)
    lane = lax.broadcasted_iota(jnp.int32, tail_b.shape, 1)
    block_rows = min(8 * tok, count * tok)

    def attend(p, carry):
        load_k(p).wait()
        load_v(p).wait()
        both = jnp.dot(kv[...], k_vmem[p], preferred_element_type=f32)
        value = jnp.dot(kv[...], v_vmem[p], preferred_element_type=f32).astype(bf16)
        rolled = pltpu.roll(both[:, NOPE:], ROPE, 1)
        low = jnp.where(lane >= ROPE, rolled, 0.0).astype(bf16)
        high = jnp.where(lane < ROPE, rolled, tail_b[...]).astype(bf16)
        key = (
            jnp.concatenate([both[:, :NOPE].astype(bf16), tail_a[...]], axis=1),
            jnp.concatenate([low, high], axis=1),
        )
        for start in range(0, count * tok, block_rows):
            at = pl.ds(start, block_rows)
            for j in range(2):
                asked = q_rows[p, at, j * LANES : (j + 2) * LANES]
                scores = lax.dot_general(
                    asked, key[j], (((1,), (1,)), ((), ())), preferred_element_type=f32
                )
                scores = scores + bias[at, :].astype(f32)
                weights = jnp.exp(scores - jnp.max(scores, axis=-1, keepdims=True))
                total = jnp.sum(weights, axis=-1, keepdims=True)
                mixed = jnp.dot(
                    weights.astype(bf16),
                    value[:, j * VDIM : (j + 1) * VDIM],
                    preferred_element_type=f32,
                )
                heads[p, at, j * VDIM : (j + 1) * VDIM] = (mixed / total).astype(bf16)
        swap(heads.at[p], heads_in.at[p], head_sem, p).start()
        return carry

    lax.fori_loop(0, pairs, attend, 0)

    def arrange(p, source, side):
        columns = pl.ds(p * 2 * VDIM, 2 * VDIM)
        x32[:, side, :, columns] = source[p].astype(f32).reshape(count, tok, 2 * VDIM)

    for p in range(pairs):
        arrange(p, heads, seq)
    for p in range(pairs):
        swap(heads.at[p], heads_in.at[p], head_sem, p).wait_recv()
        arrange(p, heads_in, 1 - seq)
    x[...] = x32[...].reshape(x.shape).astype(bf16)

    def pick(c, step, value):
        done = {bit: digit[bit] for bit in orders[c][:step]}
        done[orders[c][step]] = value
        return part.at[(c,) + tuple(done.get(bit, slice(None)) for bit in reversed(range(bits)))]

    def transfer(c, step):
        bit = orders[c][step]
        return pltpu.make_async_remote_copy(
            src_ref=pick(c, step, 1 - digit[bit]),
            dst_ref=recvs[step].at[c],
            send_sem=send_sem.at[step, c],
            recv_sem=recv_sem.at[step, c],
            device_id={"head": partner[bit]},
            device_id_type=MESH,
        )

    for c, step in plan(bits, chunks, orders):
        if step == 0:
            load_w(c).wait()
            product = jnp.dot(x[...], w_vmem[c], preferred_element_type=f32)
            part[c] = product.astype(bf16).reshape(part.shape[1:])
        else:
            transfer(c, step - 1).wait_recv()
            kept = pick(c, step - 1, digit[orders[c][step - 1]])
            total = kept[...].astype(f32) + recvs[step - 1][c].astype(f32)
            if step < bits:
                kept[...] = total.astype(bf16)
            else:
                columns = pl.ds(c * CHUNK, CHUNK)
                mine[0, :, columns] = total[:tok]
                mine[1, :, columns] = total[tok:]
        if step < bits:
            transfer(c, step).start()
    theirs[...] = mine[1 - seq].astype(bf16)
    end_swap.start()
    o_ref[:, pl.ds(pl.multiple_of(seq * half, 128), half)] = mine[seq].astype(bf16)
    end_swap.wait_recv()
    o_ref[:, pl.ds(pl.multiple_of((1 - seq) * half, 128), half)] = landed[...]
    for copy in (hid_swap, raw_swap, lat_swap, end_swap):
        copy.wait_send()
    for step in range(bits):
        for p in range(pieces):
            ql_copy(p, step).wait_send()
        lat_copy(step).wait_send()
    for p in range(pairs):
        swap(heads.at[p], heads_in.at[p], head_sem, p).wait_send()
    for c in range(chunks):
        for step in range(bits):
            transfer(c, step).wait_send()


def per_device(hidden, query_latent, kv_down, kv_gain, q_up, k_up, v_up, out_proj, block_order):
    tok = hidden.shape[0]
    head_count = lax.axis_size("head")
    seq_count = lax.axis_size("seq")
    width = kv_gain.shape[0]
    heads_dev = v_up.shape[1] // VDIM
    pairs = heads_dev // 2
    queries = head_count * tok
    bits = head_count.bit_length() - 1
    depth, half = out_proj.shape
    chunks = half // CHUNK
    orders = bit_orders(bits, chunks)
    bf16, f32 = jnp.bfloat16, jnp.float32

    blocks = angle_table(np.arange(head_count * seq_count) * tok)
    within = angle_table(np.arange(tok))

    vmem = pl.BlockSpec(memory_space=pltpu.VMEM)
    hbm = pl.BlockSpec(memory_space=pl.ANY)
    split = (2,) * bits
    unit = (2 * tok, CHUNK)
    pieces = len(gather_orders(bits))
    dma = pltpu.SemaphoreType.DMA
    return pl.pallas_call(
        functools.partial(layer_kernel, bits, chunks, orders),
        out_shape=jax.ShapeDtypeStruct((tok, 2 * half), bf16),
        in_specs=[pl.BlockSpec(memory_space=pltpu.SMEM)] + [hbm] * 10,
        out_specs=vmem,
        scratch_shapes=[
            pltpu.VMEM((3 * tok, kv_down.shape[0]), bf16),
            pltpu.VMEM(query_latent.shape, bf16),
            pltpu.VMEM((1, width), f32),
            pltpu.VMEM(blocks.shape, f32),
            pltpu.VMEM(within.shape, f32),
            pltpu.VMEM((queries, LANES), f32),
            pltpu.VMEM((queries, LANES), f32),
            pltpu.VMEM((queries, LANES), f32),
            pltpu.VMEM(kv_down.shape[::-1], bf16),
            pltpu.VMEM((pairs, q_up.shape[0], 2 * (NOPE + ROPE)), bf16),
            pltpu.VMEM((pairs, width, 2 * NOPE), bf16),
            pltpu.VMEM((pairs, width, 2 * VDIM), bf16),
            pltpu.VMEM((chunks, depth, CHUNK), bf16),
            pltpu.VMEM((tok, kv_down.shape[1]), f32),
            pltpu.VMEM((tok, kv_down.shape[1]), f32),
            pltpu.VMEM((pieces,) + split + (tok, query_latent.shape[1] // pieces), bf16),
            pltpu.VMEM((2,) + split + (tok, width + LANES), bf16),
            pltpu.VMEM((pairs, queries, 2 * (NOPE + ROPE)), bf16),
            pltpu.VMEM((queries, query_latent.shape[1]), bf16),
            pltpu.VMEM((2 * queries, width), bf16),
            pltpu.VMEM((2 * queries, LANES), bf16),
            pltpu.VMEM((2 * queries, LANES), f32),
            pltpu.VMEM((queries, 2 * queries), bf16),
            pltpu.VMEM((pairs, queries, 2 * VDIM), bf16),
            pltpu.VMEM((pairs, queries, 2 * VDIM), bf16),
            pltpu.VMEM((head_count, 2, tok, depth), f32),
            pltpu.VMEM((2 * queries, depth), bf16),
            pltpu.VMEM((chunks,) + split + unit, bf16),
        ]
        + [pltpu.VMEM((chunks,) + split[k + 1 :] + unit, bf16) for k in range(bits)]
        + [
            pltpu.VMEM((2, tok, half), f32),
            pltpu.VMEM((tok, half), bf16),
            pltpu.VMEM((tok, half), bf16),
            dma((1,)),
            dma((6,)),
            dma((pairs,)),
            dma((pairs,)),
            dma((pairs,)),
            dma((chunks,)),
            dma((bits, chunks)),
            dma((bits, chunks)),
            dma((2, 4)),
            dma((2, bits, pieces)),
            dma((2, bits, 1)),
            dma((2, pairs)),
        ],
        compiler_params=pltpu.CompilerParams(
            collective_id=1, has_side_effects=True, vmem_limit_bytes=VMEM_BYTES
        ),
    )(
        block_order, hidden, query_latent, kv_down.T, kv_gain[None, :], q_up, k_up, v_up, out_proj,
        blocks, within,
    )


def solution(mesh):
    placed = (
        P(("groups", "head", "seq"), None),
        P(("groups", "head", "seq"), None),
        P("seq", None),
        P(),
        P(None, "head"),
        P(None, "head"),
        P(None, "head"),
        P("head", "seq"),
        P("groups"),
    )
    return jax.shard_map(
        per_device,
        mesh=mesh,
        in_specs=placed,
        out_specs=P(("groups", "head", "seq"), None),
        check_vma=False,
    )
```
